32 devices in a mesh: pairs: 8 (over y, x, core), dates: 4 (over z).
Axes of the slice: x: 2, y: 2, z: 4, core: 2. Of those that a mesh axis runs over, the one named last changes fastest.
Arguments:
- returns: bfloat16 [4096, 4096], P('dates', 'pairs'), may hold values from -16 to 16
- plan: int32 [3, 8], P(None, 'pairs'), may hold values from 0 to 1
Outputs:
- rotated_panel: bfloat16 [4096, 4096], P('dates', 'pairs')
- disorder: float32 [3], replicated
The draws below stay inside these ranges and needn't reach their ends.
All inputs are finite; a program needn't handle non-finite values.
Results may differ from the reference program's by a relative error of at most 0.0067.
Values may be sent and summed in bfloat16 or wider, within the bound.
No kernel may reach another device: no remote copies, remote signals or barrier semaphores. Data moves between devices by JAX's collectives and lax.ppermute only.
A program may use at most 64 MiB of HBM per device.

```python
import jax
import jax.numpy as jnp
from jax import lax

B = 256
ROUNDS = 3
NS_STEPS = 3
ROWS = 4096
SERIES = 4096
N_PAIRS = 8


def draw_returns(key, part):
    key_factor, key_loading, key_strength, key_noise_scale, key_noise = jax.random.split(jax.random.fold_in(key, 17), 5)
    factors = jax.random.normal(key_factor, (ROWS, 8), jnp.float32)
    loadings = jax.random.normal(key_loading, (SERIES, 8), jnp.float32)
    position = jnp.arange(SERIES, dtype=jnp.float32) / SERIES
    strength = (0.3 + 1.2 * position) * jax.random.uniform(key_strength, (SERIES,), jnp.float32, 0.5, 1.5)
    noise_scale = jnp.exp(jax.random.uniform(key_noise_scale, (SERIES,), jnp.float32, -0.7, 0.7))
    noise = jax.random.normal(key_noise, (ROWS, SERIES), jnp.float32)
    common = jnp.dot(factors, loadings.T) * (strength / jnp.sqrt(8.0))[None, :]
    values = common + noise * noise_scale[None, :]
    return jnp.clip(values, -16.0, 16.0).astype(jnp.bfloat16)


def touch_ends(values, rng, smallest, largest):
    place = [jax.random.randint(jax.random.fold_in(rng, axis), (), 0, length) for axis, length in enumerate(values.shape)]
    widest = values.shape.index(max(values.shape))
    neighbour = place[:widest] + [(place[widest] + 1) % values.shape[widest]] + place[widest + 1:]
    return values.at[tuple(place)].set(smallest).at[tuple(neighbour)].set(largest)


def setup_inputs(seed: int = 0) -> dict:
    arg_keys = jax.random.split(jax.random.key(seed), 3)
    returns = draw_returns(jax.random.fold_in(arg_keys[2], 71), 0)
    plan = touch_ends(jax.random.randint(arg_keys[1], (ROUNDS, N_PAIRS), 0, 2), jax.random.fold_in(arg_keys[1], 1), 0, 1).astype(jnp.int32)
    return {"returns": returns, "plan": plan}


damping_base = 0.5
epsilon = 1e-06

def reference(returns, plan):
    highest = lax.Precision.HIGHEST
    blocks = returns.reshape(ROWS, N_PAIRS, 2, B).transpose(1, 2, 0, 3)
    identity = jnp.eye(2 * B, dtype=jnp.float32)
    history = []
    for step_index in range(ROUNDS):
        joined = jnp.concatenate([blocks[:, 0], blocks[:, 1]], axis=2).astype(jnp.float32)
        gram = jnp.einsum('pmi,pmj->pij', joined, joined, precision=highest)
        diag_sum = jnp.diagonal(gram, axis1=1, axis2=2) + epsilon
        col_scale = jnp.sqrt(diag_sum)
        cross_block = gram[:, :B, B:] / (col_scale[:, :B, None] * col_scale[:, None, B:])
        coupling = lax.optimization_barrier(jnp.sum(cross_block * cross_block, axis=(1, 2)))
        overall = jnp.sum(coupling / (B * B))
        history.append(overall)
        damping = damping_base / jnp.sqrt(1.0 + B * B * overall / N_PAIRS)
        zeros_block = jnp.zeros_like(cross_block)
        skew_part = jnp.concatenate([jnp.concatenate([zeros_block, -cross_block], axis=2), jnp.concatenate([jnp.transpose(cross_block, (0, 2, 1)), zeros_block], axis=2)], axis=1)
        factor = (identity + damping * skew_part) / jnp.sqrt(1.0 + 2.0 * damping * damping * coupling)[:, None, None]
        for inner_step in range(NS_STEPS):
            squared = jnp.einsum('pab,pac->pbc', factor, factor, precision=highest)
            factor = 1.5 * factor - 0.5 * jnp.einsum('pab,pbc->pac', factor, squared, precision=highest)
        rotation = lax.optimization_barrier(factor.astype(jnp.bfloat16)).astype(jnp.float32)
        rotated = jnp.einsum('pmi,pij->pmj', joined, rotation, precision=highest).astype(jnp.bfloat16)
        front_half = rotated[:, :, :B]
        back_half = rotated[:, :, B:]
        chosen = plan[step_index][:, None, None]
        outgoing = jnp.where(chosen == 0, front_half, back_half)
        incoming = jnp.roll(outgoing, 1, axis=0)
        slot_zero = jnp.where(chosen == 0, incoming, front_half)
        slot_one = jnp.where(chosen == 1, incoming, back_half)
        blocks = jnp.stack([slot_zero, slot_one], axis=1)
    rotated_panel = blocks.transpose(2, 0, 1, 3).reshape(ROWS, SERIES)
    return (rotated_panel, jnp.stack(history))
```

```python
import jax
import jax.numpy as jnp
from jax import lax
from jax.experimental import pallas as pl
from jax.experimental.pallas import tpu as pltpu
from jax.sharding import PartitionSpec as P

damping_base = 0.5
epsilon = 1e-06
TAIL = 16
F32 = jnp.float32
BF16 = jnp.bfloat16


def shifted(x, axis, by):
    devices = lax.axis_size(axis)
    return lax.ppermute(x, axis, [(i, (i + by) % devices) for i in range(devices)])


def swapped(x, axis, mask):
    return lax.ppermute(x, axis, [(i, i ^ mask) for i in range(lax.axis_size(axis))])


def sum_over(x, axis):
    devices = lax.axis_size(axis)
    if devices & (devices - 1):
        return lax.psum(x, axis)
    stride = 1
    while stride < devices:
        left = devices // stride
        if left >= 4 and (left.bit_length() - 1) % 2 == 0:
            a, b, c = (swapped(x, axis, stride * k) for k in (1, 2, 3))
            x = (x + a) + (b + c)
            stride *= 4
        else:
            x = x + swapped(x, axis, stride)
            stride *= 2
    return x


def call(body, outs, args, scratch=()):
    specs = [
        pl.BlockSpec(memory_space=pltpu.SMEM if a.dtype == jnp.int32 else pltpu.VMEM) for a in args
    ]
    return pl.pallas_call(
        body,
        out_shape=outs,
        in_specs=specs,
        out_specs=jax.tree.map(lambda _: pl.BlockSpec(memory_space=pltpu.VMEM), outs),
        scratch_shapes=scratch,
        compiler_params=pltpu.CompilerParams(vmem_limit_bytes=40 << 20),
    )(*args)


def message_like(b):
    return jax.ShapeDtypeStruct((b + TAIL, b), BF16)


def split_rows(rows):
    b = rows[0].shape[1]
    at = lax.broadcasted_iota(jnp.int32, (TAIL, b), 0)
    tail = jnp.zeros((TAIL, b), F32)
    for i, row in enumerate(rows):
        high = row.astype(BF16).astype(F32)
        tail = jnp.where(at == 2 * i, high, tail)
        tail = jnp.where(at == 2 * i + 1, row - high, tail)
    return tail.astype(BF16)


def joined_rows(ref, count):
    b = ref.shape[1]
    tail = ref[b:, :].astype(F32)
    return [tail[2 * i : 2 * i + 1] + tail[2 * i + 1 : 2 * i + 2] for i in range(count)]


def write_gram(panel_ref, out_ref):
    b = out_ref.shape[1]
    rows = panel_ref.shape[0]
    step = min(rows, 256)
    cross = jnp.zeros((b, b), F32)
    left_sq = jnp.zeros((1, b), F32)
    right_sq = jnp.zeros((1, b), F32)
    for start in range(0, rows, step):
        left = panel_ref[start : start + step, :b]
        right = panel_ref[start : start + step, b:]
        cross += lax.dot_general(left, right, (((0,), (0,)), ((), ())), preferred_element_type=F32)
        left32 = left.astype(F32)
        right32 = right.astype(F32)
        left_sq += jnp.sum(left32 * left32, axis=0, keepdims=True)
        right_sq += jnp.sum(right32 * right32, axis=0, keepdims=True)
    out_ref[:b, :] = cross.astype(BF16)
    out_ref[b:, :] = split_rows([left_sq, right_sq])


def gram_kernel(panel_ref, out_ref):
    write_gram(panel_ref, out_ref)


def add_kernel(mine_ref, other_ref, out_ref):
    b = out_ref.shape[1]
    out_ref[:b, :] = (mine_ref[:b, :].astype(F32) + other_ref[:b, :].astype(F32)).astype(BF16)
    sums = [m + o for m, o in zip(joined_rows(mine_ref, 2), joined_rows(other_ref, 2))]
    out_ref[b:, :] = split_rows(sums)


def cross_kernel(mine_ref, other_ref, out_ref, coupling_ref):
    b = out_ref.shape[1]
    left_sq, right_sq = (
        m + o + epsilon for m, o in zip(joined_rows(mine_ref, 2), joined_rows(other_ref, 2))
    )
    gram = mine_ref[:b, :].astype(F32) + other_ref[:b, :].astype(F32)
    on_diagonal = lax.broadcasted_iota(jnp.int32, (b, b), 0) == lax.broadcasted_iota(
        jnp.int32, (b, b), 1
    )
    left_col = jnp.sum(jnp.where(on_diagonal, left_sq, 0.0), axis=1, keepdims=True)
    cross = gram / (jnp.sqrt(left_col) * jnp.sqrt(right_sq))
    coupling = jnp.sum(jnp.sum(cross * cross, axis=0, keepdims=True), axis=1, keepdims=True)
    out_ref[:b, :] = cross.astype(BF16)
    out_ref[b:, :] = split_rows([jnp.broadcast_to(coupling, (1, b))])
    coupling_ref[...] = jnp.broadcast_to(coupling, coupling_ref.shape)


def bdot(x, y):
    return jnp.dot(x.astype(BF16), y.astype(BF16), preferred_element_type=F32)


def columns_of_rotation(cross_ref, total, pairs_count, slot, out_ref):
    b = out_ref.shape[1]
    (coupling,) = joined_rows(cross_ref, 1)
    damping = damping_base / jnp.sqrt(1.0 + total / pairs_count)
    scale = 1.0 / jnp.sqrt(1.0 + 2.0 * damping * damping * coupling)
    cross = cross_ref[:b, :].astype(F32)
    turned = cross.T
    first = slot == 0
    k = jnp.where(first, turned, -cross).astype(BF16)
    k_t = jnp.where(first, cross, -turned).astype(BF16)
    alpha = scale * scale
    n1 = (alpha * damping * damping) * jnp.dot(k_t, k, preferred_element_type=F32)
    n2 = bdot(n1, n1)
    n3 = bdot(n2, n1)
    n4 = bdot(n2, n2)

    def taylor(y):
        return y * (2.25 + y * (0.25 * y - 1.5)), 2.25 + y * (0.75 * y - 3.0), 0.75 * y - 1.5

    y1, slope, bend = taylor(alpha)
    gain1 = 1.5 - 0.5 * alpha
    gain2 = 1.5 - 0.5 * y1
    d1 = slope * n1 + bend * n2 + 0.25 * n3
    gain12 = gain1 * gain2
    d12 = (
        (-0.5 * gain2 - 0.5 * gain1 * slope) * n1
        + (0.25 * slope - 0.5 * gain1 * bend) * n2
        + (0.25 * bend - 0.125 * gain1) * n3
        + 0.0625 * n4
    )
    y2, slope, bend = taylor(y1)
    square = bdot(d1, d1)
    d2 = slope * d1 + bend * square + 0.25 * bdot(d1, square)
    gain3 = 1.5 - 0.5 * y2
    gain = gain12 * gain3
    delta = gain3 * d12 - 0.5 * gain12 * d2 - 0.5 * bdot(d12, d2)
    on_diagonal = lax.broadcasted_iota(jnp.int32, (b, b), 0) == lax.broadcasted_iota(
        jnp.int32, (b, b), 1
    )
    own = scale * (jnp.where(on_diagonal, gain, 0.0) + delta)
    off = (scale * damping) * (gain * k.astype(F32) + bdot(k, delta))
    out_ref[pl.ds(pl.multiple_of(slot * b, b), b), :] = own.astype(BF16)
    out_ref[pl.ds(pl.multiple_of((1 - slot) * b, b), b), :] = off.astype(BF16)


def turn_kernel(pairs_count, slots_ref, total_ref, cross_ref, before_ref, panel_ref, previous_ref,
                out_ref, *rest):
    *gram_ref, stay_ref, move_ref = rest
    b = stay_ref.shape[1]
    mine = slots_ref[0]
    theirs = slots_ref[1]
    total = jnp.concatenate([total_ref[0:1, :]] * (b // total_ref.shape[1]), axis=1)
    columns_of_rotation(cross_ref, total, pairs_count, 1 - mine, stay_ref)
    columns_of_rotation(before_ref, total, pairs_count, theirs, move_ref)
    rows = out_ref.shape[0]
    step = min(rows, 256)
    for start in range(0, rows, step):
        at = slice(start, start + step)
        stay = jnp.dot(panel_ref[at, :], stay_ref[...], preferred_element_type=F32).astype(BF16)
        move = jnp.dot(previous_ref[at, :], move_ref[...], preferred_element_type=F32).astype(BF16)

        @pl.when(mine == 0)
        def _():
            out_ref[at, :b] = move
            out_ref[at, b:] = stay

        @pl.when(mine != 0)
        def _():
            out_ref[at, :b] = stay
            out_ref[at, b:] = move

    if gram_ref:
        write_gram(out_ref, gram_ref[0])


def local(returns, plan):
    pairs_count = lax.axis_size("pairs")
    dates_count = lax.axis_size("dates")
    rounds = plan.shape[0]
    rows, width = returns.shape
    b = width // 2
    slots = jnp.concatenate([plan, shifted(plan, "pairs", 1)], axis=1)
    panel = returns
    message = call(gram_kernel, message_like(b), [panel])
    history = []
    for step_index in range(rounds):
        previous = shifted(panel, "pairs", 1)
        stride = 1
        while 2 * stride < dates_count:
            message = call(
                add_kernel, message_like(b), [message, swapped(message, "dates", stride)]
            )
            stride *= 2
        cross, coupling = call(
            cross_kernel,
            [message_like(b), jax.ShapeDtypeStruct((8, 128), F32)],
            [message, swapped(message, "dates", stride)],
        )
        before = shifted(cross, "pairs", 1)
        total = sum_over(coupling, "pairs")
        history.append(total[0, 0] / (b * b))
        outs = [jax.ShapeDtypeStruct((rows, width), BF16)]
        if step_index + 1 < rounds:
            outs.append(message_like(b))
        panel, *message = call(
            lambda *refs: turn_kernel(pairs_count, *refs),
            outs,
            [slots[step_index], total, cross, before, panel, previous],
            [pltpu.VMEM((width, b), BF16), pltpu.VMEM((width, b), BF16)],
        )
        if message:
            message = message[0]
    return (panel, jnp.stack(history))


def solution(mesh):
    return jax.shard_map(
        local,
        mesh=mesh,
        in_specs=(P("dates", "pairs"), P(None, "pairs")),
        out_specs=(P("dates", "pairs"), P()),
        check_vma=False,
    )
```
